128 devices in a mesh: seq: 8 (over y_lo, x), tp: 8 (over z, core), grp: 2 (over y_hi).
Axes of the slice: x: 4, y: 4 (y_hi: 2, y_lo: 2; y = y_hi * 2 + y_lo), z: 4, core: 2. Of those that a mesh axis runs over, the one named last changes fastest.
Arguments:
- query: bfloat16 [16, 64, 8192], P('grp', None, 'tp'), parts along dimension 0, may hold values from -15 to 15
- cache: bfloat16 [16, 16384, 8, 256], P('grp', 'tp', 'seq'), parts along dimension 0, may hold values from -6 to 6
- head_of_slot: int32 [16], P('grp'), parts along dimension 0, may hold values from 0 to 7, each once
- lengths: int32 [16], P('grp'), parts along dimension 0, may hold values from 8192 to 16384
- out_weight: bfloat16 [8192, 8192], P('tp', 'seq'), may hold values from -0.0625 to 0.0625
Outputs:
- projected: bfloat16 [16, 64, 8192], P(('grp', 'tp'), None, 'seq'), parts along dimension 0
The draws below stay inside these ranges and needn't reach their ends.
There are 2 independent parts, one for each index of `grp`. The reference program is written for one: setup_inputs(seed, part) draws one part's arguments, and reference() takes and returns one part's arrays. A program takes and returns all parts, laid end to end along the dimension named above; an argument that names none is the same for every part. Nothing has to cross between parts.
Inputs may be any that keep to these rules, and one draw needn't show every extreme that they name: head_of_slot names every KV head exactly once.
All inputs are finite; a program needn't handle non-finite values.
Results may differ from the reference program's by a relative error of at most 0.01.
Values may be sent and summed in bfloat16 or wider, within the bound.
No kernel may reach another device: no remote copies, remote signals or barrier semaphores. Data moves between devices by JAX's collectives and lax.ppermute only.
A program may use at most 128 MiB of HBM per device.

```python
import math
import jax
import jax.numpy as jnp
from jax import lax

D = 8192
HQ = 64
KVH = 8
HD = 128
B = 8
QT = 64
L = 16384


def draw_query(key, part):
    own_key = jax.random.fold_in(key, 11)
    values = jnp.clip(3.0 * jax.random.normal(own_key, (B, QT, HQ * HD), jnp.float32), -15.0, 15.0)
    return values.astype(jnp.bfloat16)


def draw_cache(key, part):
    own_key = jax.random.fold_in(key, 23)
    values = jnp.clip(jax.random.normal(own_key, (B, L, KVH, 2 * HD), jnp.float32), -6.0, 6.0)
    return values.astype(jnp.bfloat16)


def with_ends(values, key, smallest, top_value):
    shape = values.shape
    spot = [jax.random.randint(jax.random.fold_in(key, axis), (), 0, shape[axis]) for axis in range(len(shape))]
    values = values.at[tuple(spot)].set(smallest)
    longest = shape.index(max(shape))
    spot[longest] = (spot[longest] + 1) % shape[longest]
    return values.at[tuple(spot)].set(top_value)


def shard_levels(stream_key, extent, shards, smallest, top_value):
    factor_of = 1.0
    for position, parts in shards:
        heights = jax.random.uniform(jax.random.fold_in(jax.random.fold_in(stream_key, 6), position), (parts,), jnp.float32, smallest / len(shards), top_value / len(shards))
        factor_of = factor_of * jnp.repeat(jnp.exp(heights), extent[position] // parts).reshape((-1,) + (1,) * (len(extent) - 1 - position))
    return factor_of


def noise(key, shape, spread, bound, cuts=(), kind=jnp.bfloat16):
    loudness = shard_levels(key, shape, cuts, -0.22, 0.18) if cuts else 1.0
    drawn = jax.random.normal(key, shape, jnp.float32) * spread * loudness
    return jnp.minimum(jnp.maximum(drawn, -bound), bound).astype(kind)


def setup_inputs(seed: int = 0, part: int = 0) -> dict:
    arg_keys = jax.random.split(jax.random.key(seed), 6)
    own_keys = jax.random.split(jax.random.fold_in(arg_keys[5], part), 6)
    query = draw_query(jax.random.fold_in(jax.random.fold_in(arg_keys[5], part), 71), part)
    cache = draw_cache(jax.random.fold_in(jax.random.fold_in(arg_keys[5], part), 71), part)
    head_of_slot = jax.random.permutation(own_keys[2], KVH).astype(jnp.int32)
    lengths = with_ends(jax.random.randint(own_keys[3], (B,), L // 2, L + 1), jax.random.fold_in(own_keys[3], 1), L // 2, L).astype(jnp.int32)
    out_weight = noise(arg_keys[4], (HQ * HD, D), (HQ * HD) ** -0.5, 0.0625, ((0, 8), (1, 8)))
    return dict(query=query, cache=cache, head_of_slot=head_of_slot, lengths=lengths, out_weight=out_weight)


MASKED_SCORE = -1e+30

def reference(query, cache, head_of_slot, lengths, out_weight):
    group_size = HQ // KVH
    scaling = 1.0 / math.sqrt(HD)
    slot_ids = jnp.arange(KVH, dtype=jnp.int32)
    slot_of_head = lax.optimization_barrier(jnp.sum(jnp.where(head_of_slot[None, :] == slot_ids[:, None], slot_ids[None, :], 0), axis=1)).astype(jnp.int32)
    positions = jnp.arange(L, dtype=jnp.int32)
    row_token = jnp.arange(QT * group_size, dtype=jnp.int32) // group_size

    def attend_pair(pair_index):
        seq_index = pair_index // KVH
        kv_head = pair_index % KVH
        entries = lax.dynamic_index_in_dim(cache, seq_index, 0, False)
        entries = lax.dynamic_index_in_dim(entries, slot_of_head[kv_head], 1, False)
        queries = lax.dynamic_index_in_dim(query, seq_index, 0, False)
        queries = lax.dynamic_slice_in_dim(queries, kv_head * group_size * HD, group_size * HD, 1)
        queries = queries.reshape(QT * group_size, HD)
        scores = jnp.dot(queries, entries[:, :HD].T, preferred_element_type=jnp.float32) * scaling
        limits = lengths[seq_index] - QT + row_token
        visible = positions[None, :] <= limits[:, None]
        scores = jnp.where(visible, scores, MASKED_SCORE)
        maxima = lax.optimization_barrier(jnp.max(scores, axis=1))
        weights = jnp.where(visible, jnp.exp(scores - maxima[:, None]), 0.0)
        totals = lax.optimization_barrier(jnp.sum(weights, axis=1))
        blended = jnp.dot(weights.astype(jnp.bfloat16), entries[:, HD:], preferred_element_type=jnp.float32)
        return (blended / totals[:, None]).astype(jnp.bfloat16).reshape(QT, group_size * HD)
    attended = lax.map(attend_pair, jnp.arange(B * KVH, dtype=jnp.int32))
    attended = attended.reshape(B, KVH, QT, group_size * HD).transpose(0, 2, 1, 3).reshape(B * QT, HQ * HD)
    projected = jnp.dot(attended, out_weight, preferred_element_type=jnp.float32)
    return projected.astype(jnp.bfloat16).reshape(B, QT, D)
```

```python
import functools
import math

import jax
import jax.numpy as jnp
from jax import lax
from jax.experimental import pallas as pl
from jax.experimental.pallas import tpu as pltpu
from jax.sharding import PartitionSpec as P


KVH = 8
HD = 128
MASKED = -1e30
LOG2E = math.log2(math.e)
EXTRA = 128


def split3(x):
    hi = x.astype(jnp.bfloat16)
    rest = x - hi.astype(jnp.float32)
    mid = rest.astype(jnp.bfloat16)
    low = (rest - mid.astype(jnp.float32)).astype(jnp.bfloat16)
    return hi, mid, low


def joined(ext):
    return ext + (pltpu.roll(ext, EXTRA - 8, 1) + pltpu.roll(ext, EXTRA - 16, 1))


def packed(lse):
    lane = lax.broadcasted_iota(jnp.int32, lse.shape, 1)
    hi, mid, low = (part.astype(jnp.float32) for part in split3(lse))
    out = jnp.where(lane < 8, hi, 0.0)
    out = jnp.where((lane >= 8) & (lane < 16), pltpu.roll(mid, 8, 1), out)
    out = jnp.where((lane >= 16) & (lane < 24), pltpu.roll(low, 16, 1), out)
    return out.astype(jnp.bfloat16)


def attention_body(meta, q_ref, kv_ref, out_ref, *, block, group):
    tokens = q_ref.shape[1]
    extent = kv_ref.shape[1]
    seq = 2 * pl.program_id(0) + meta[0]
    first = meta[1] * extent
    length = meta[2 + seq]
    c2 = LOG2E / math.sqrt(HD)
    rows = tokens * group

    def compute(masked):
        q = jnp.concatenate([q_ref[0, :, HD * h : HD * (h + 1)] for h in range(group)], axis=0)
        top = None
        for at in range(0, extent, block):
            scores = lax.dot_general(
                q,
                kv_ref[0, at : at + block, :HD],
                (((1,), (1,)), ((), ())),
                preferred_element_type=jnp.float32,
            )
            if masked:
                pos = first + at + lax.broadcasted_iota(jnp.int32, (tokens, block), 1)
                limit = length - tokens + lax.broadcasted_iota(jnp.int32, (tokens, block), 0)
                visible = jnp.concatenate([pos <= limit] * group, axis=0)
                scores = jnp.where(visible, scores, MASKED)
            here = jnp.max(scores, axis=1, keepdims=True)
            new_top = here if top is None else jnp.maximum(top, here)
            weights = jnp.exp2((scores - new_top) * c2)
            if masked:
                weights = jnp.where(visible, weights, 0.0)
            values = kv_ref[0, at : at + block, HD:]
            both = jnp.concatenate([values, jnp.ones_like(values)], axis=1)
            sums = jnp.dot(weights.astype(jnp.bfloat16), both, preferred_element_type=jnp.float32)
            part, part_total = sums[:, :HD], sums[:, HD:]
            if top is None:
                blended, totals = part, part_total
            else:
                shrink = jnp.exp2((top - new_top) * c2)
                blended = blended * shrink + part
                totals = totals * shrink + part_total
            top = new_top
        if masked:
            totals = jnp.where(totals > 0.0, totals, 1.0)
        normal = (blended / totals).astype(jnp.bfloat16)
        lse = top * c2 + jnp.log2(totals)
        lane = lax.broadcasted_iota(jnp.int32, (tokens, EXTRA), 1)
        gathered = jnp.zeros((tokens, EXTRA), jnp.float32)
        for h in range(group):
            out_ref[0, :, HD * h : HD * (h + 1)] = normal[tokens * h : tokens * (h + 1)]
            gathered = jnp.where(lane == h, lse[tokens * h : tokens * (h + 1)], gathered)
        out_ref[0, :, HD * group :] = packed(gathered)

    full = first + extent - 1 <= length - tokens
    hidden = first > length - 1

    @pl.when(full)
    def _():
        compute(False)

    @pl.when(jnp.logical_not(full | hidden))
    def _():
        compute(True)

    @pl.when(hidden)
    def _():
        out_ref[0, :, : HD * group] = jnp.zeros((tokens, HD * group), jnp.bfloat16)
        lane = lax.broadcasted_iota(jnp.int32, (tokens, EXTRA), 1)
        out_ref[0, :, HD * group :] = jnp.where(lane < 8, MASKED, 0.0).astype(jnp.bfloat16)


def attention(meta, q, kv, group):
    count, tokens, width = q.shape
    extent = kv.shape[1]
    return pl.pallas_call(
        functools.partial(attention_body, block=256, group=group),
        grid_spec=pltpu.PrefetchScalarGridSpec(
            num_scalar_prefetch=1,
            grid=(count,),
            in_specs=[
                pl.BlockSpec((1, tokens, width), lambda i, m: (i, 0, 0)),
                pl.BlockSpec((1, extent, 2 * HD), lambda i, m: (2 * i + m[0], 0, 0)),
            ],
            out_specs=pl.BlockSpec((1, tokens, width + EXTRA), lambda i, m: (i, 0, 0)),
        ),
        out_shape=jax.ShapeDtypeStruct((count, tokens, width + EXTRA), jnp.bfloat16),
        compiler_params=pltpu.CompilerParams(vmem_limit_bytes=48 * 1024 * 1024),
        cost_estimate=pl.CostEstimate(
            flops=count * tokens * group * extent * HD * 4,
            bytes_accessed=count * extent * 2 * HD * 2,
            transcendentals=count * tokens * group * extent,
        ),
        name="attend",
    )(meta, q, kv)


def merge_shares(parts):
    top = functools.reduce(jnp.maximum, parts)
    weights = [jnp.exp2(part - top) for part in parts]
    total = functools.reduce(jnp.add, weights)
    return [w / total for w in weights], top + jnp.log2(total)


def merge_pair_body(a_ref, b_ref, out_ref, *, group):
    a, b = (joined(ref[0, :, HD * group :].astype(jnp.float32)) for ref in (a_ref, b_ref))
    (share_a, share_b), lse = merge_shares([a, b])
    for h in range(group):
        cut = slice(HD * h, HD * (h + 1))
        out_ref[0, :, cut] = (
            a_ref[0, :, cut].astype(jnp.float32) * share_a[:, h : h + 1]
            + b_ref[0, :, cut].astype(jnp.float32) * share_b[:, h : h + 1]
        ).astype(jnp.bfloat16)
    out_ref[0, :, HD * group :] = packed(lse)


def merge_pair(a, b, group):
    spec = pl.BlockSpec((1,) + a.shape[1:], lambda i: (i, 0, 0))
    return pl.pallas_call(
        functools.partial(merge_pair_body, group=group),
        grid=(a.shape[0],),
        in_specs=[spec, spec],
        out_specs=spec,
        out_shape=jax.ShapeDtypeStruct(a.shape, jnp.bfloat16),
        cost_estimate=pl.CostEstimate(flops=4 * a.size, bytes_accessed=6 * a.size, transcendentals=0),
        name="merge_pair",
    )(a, b)


def merge_all_body(x_ref, out_ref, *, group):
    count = x_ref.shape[0]
    shares, _ = merge_shares([joined(x_ref[k, :, HD * group :].astype(jnp.float32)) for k in range(count)])
    for h in range(group):
        cut = slice(HD * h, HD * (h + 1))
        total = x_ref[0, :, cut].astype(jnp.float32) * shares[0][:, h : h + 1]
        for k in range(1, count):
            total = total + x_ref[k, :, cut].astype(jnp.float32) * shares[k][:, h : h + 1]
        out_ref[h] = total.astype(jnp.bfloat16)


def merge_all(x, group):
    return pl.pallas_call(
        functools.partial(merge_all_body, group=group),
        out_shape=jax.ShapeDtypeStruct((group, x.shape[1], HD), jnp.bfloat16),
        cost_estimate=pl.CostEstimate(flops=2 * x.size, bytes_accessed=3 * x.size, transcendentals=0),
        name="merge_all",
    )(x)


def reorder_body(table, x_ref, out_ref):
    for h in range(x_ref.shape[0]):
        out_ref[h] = x_ref[table[h]]


def reorder(table, x):
    return pl.pallas_call(
        reorder_body,
        grid_spec=pltpu.PrefetchScalarGridSpec(
            num_scalar_prefetch=1,
            grid=(1,),
            in_specs=[pl.BlockSpec(x.shape, lambda i, m: (0,) * x.ndim)],
            out_specs=pl.BlockSpec(x.shape, lambda i, m: (0,) * x.ndim),
        ),
        out_shape=jax.ShapeDtypeStruct(x.shape, x.dtype),
        cost_estimate=pl.CostEstimate(flops=x.size, bytes_accessed=4 * x.size, transcendentals=0),
        name="reorder",
    )(table, x)


def project_body(meta, *refs):
    *pieces, w_ref, out_ref = refs
    count = len(pieces)
    tokens = pieces[0].shape[2]
    half = pieces[0].shape[0]
    x = jnp.concatenate([ref[:, meta[0]].reshape(half * tokens, HD) for ref in pieces], axis=1)
    rank = meta[1]
    w = jnp.concatenate(
        [w_ref[pl.ds(pl.multiple_of((rank ^ k) * HD, HD), HD), :] for k in range(count)], axis=0
    )
    y = jnp.dot(x, w, preferred_element_type=jnp.float32)
    out_ref[...] = y.astype(jnp.bfloat16).reshape(out_ref.shape)


def project(meta, pieces, w):
    half, _, tokens, _ = pieces[0].shape
    width = w.shape[1]
    cut = 256
    return pl.pallas_call(
        project_body,
        grid_spec=pltpu.PrefetchScalarGridSpec(
            num_scalar_prefetch=1,
            grid=(width // cut,),
            in_specs=[pl.BlockSpec(p.shape, lambda i, m: (0, 0, 0, 0)) for p in pieces]
            + [pl.BlockSpec((w.shape[0], cut), lambda i, m: (0, i))],
            out_specs=pl.BlockSpec((half, tokens, cut), lambda i, m: (0, 0, i)),
        ),
        out_shape=jax.ShapeDtypeStruct((half, tokens, width), jnp.bfloat16),
        cost_estimate=pl.CostEstimate(
            flops=2 * half * tokens * w.size, bytes_accessed=2 * w.size, transcendentals=0
        ),
        name="project",
    )(meta, *pieces, w)


def slot_table(head_of_slot):
    slot_ids = jnp.arange(head_of_slot.shape[0], dtype=jnp.int32)
    return jnp.sum(
        jnp.where(head_of_slot[None, :] == slot_ids[:, None], slot_ids[None, :], 0), axis=1
    ).astype(jnp.int32)


def local(query, cache, head_of_slot, lengths, out_weight):
    seqs, tokens, width = query.shape
    group = width // HD
    pairs = seqs // 2
    seq_rank = lax.axis_index("seq")
    rank = lax.axis_index("tp")
    core, z = rank % 2, rank // 2
    chips = lax.axis_size("tp") // 2
    seq_size = lax.axis_size("seq")
    head = head_of_slot[seq_rank]
    slot_of_head = slot_table(head_of_slot)
    kv = cache.reshape(seqs, cache.shape[1], cache.shape[3])

    swap_core = [(i, i ^ 1) for i in range(2 * chips)]
    flip, mirror = (lambda v: v ^ 1), (lambda v: chips - 1 - v)
    first_hop = [(2 * v + c, 2 * (flip, mirror)[c](v) + c) for v in range(chips) for c in range(2)]
    second_hop = [(2 * v + c, 2 * (mirror, flip)[c](v) + c) for v in range(chips) for c in range(2)]

    by_parity = query.reshape(pairs, 2, tokens, width)

    def parity(x, which):
        return lax.dynamic_index_in_dim(x, which, 1, keepdims=False)

    mine = parity(by_parity, 1 - core)
    other = lax.ppermute(parity(by_parity, core), "tp", swap_core)
    root = head // 2
    here = jnp.where(head % 2 == core, mine, other)
    partner = jnp.where(core == 0, z ^ 1, chips - 1 - z)
    came = lax.ppermute(here, "tp", first_hop)
    here = jnp.where(partner == root, came, here)
    came = lax.ppermute(here, "tp", second_hop)
    here = jnp.where((z == root) | (partner == root), here, came)
    rest = lax.ppermute(here, "tp", swap_core)

    facts = lambda which: jnp.concatenate([jnp.stack([which, rank]).astype(jnp.int32), lengths])
    sent = attention(facts(1 - core), here, kv, group)
    came = lax.ppermute(sent, "tp", swap_core)
    kept = attention(facts(core), rest, kv, group)
    chip_sum = merge_pair(kept, came, group)

    z_groups = [[2 * v + c for v in range(chips)] for c in range(2)]
    arrived = lax.all_to_all(chip_sum, "tp", 0, 0, tiled=True, axis_index_groups=z_groups)
    by_query_head = merge_all(arrived, group)

    by_slot = lax.all_to_all(by_query_head, "seq", 0, 0, tiled=True)
    by_head = reorder(slot_of_head, by_slot)
    piece = lax.all_to_all(by_head, "tp", 0, 0, tiled=True)
    pieces = [piece] + [
        lax.ppermute(piece, "seq", [(i, i ^ k) for i in range(seq_size)]) for k in range(1, seq_size)
    ]
    pieces = [p.reshape(pairs, 2, tokens, HD) for p in pieces]

    pick = lambda which: jnp.stack([which, seq_rank]).astype(jnp.int32)
    sent = project(pick(1 - core), pieces, out_weight)
    came = lax.ppermute(sent, "tp", swap_core)
    kept = project(pick(core), pieces, out_weight)
    chip_sum = (kept.astype(jnp.float32) + came.astype(jnp.float32)).astype(jnp.bfloat16)
    arrived = lax.all_to_all(chip_sum, "tp", 0, 0, tiled=True, axis_index_groups=z_groups)
    return jnp.sum(arrived.astype(jnp.float32), axis=0, keepdims=True).astype(jnp.bfloat16)


def solution(mesh):
    in_specs = (
        P("grp", None, "tp"),
        P("grp", "tp", "seq", None),
        P("grp"),
        P("grp"),
        P("tp", "seq"),
    )
    out_specs = P(("grp", "tp"), None, "seq")
    return jax.shard_map(local, mesh=mesh, in_specs=in_specs, out_specs=out_specs, check_vma=False)
```

```python
import functools
import math

import jax
import jax.numpy as jnp
from jax import lax
from jax.experimental import pallas as pl
from jax.experimental.pallas import tpu as pltpu
from jax.sharding import PartitionSpec as P


KVH = 8
HD = 128
MASKED = -1e30
LOG2E = math.log2(math.e)
EXTRA = 128
CHUNKS = 2


def split3(x):
    hi = x.astype(jnp.bfloat16)
    rest = x - hi.astype(jnp.float32)
    mid = rest.astype(jnp.bfloat16)
    low = (rest - mid.astype(jnp.float32)).astype(jnp.bfloat16)
    return hi, mid, low


def joined(ext):
    return ext + (pltpu.roll(ext, EXTRA - 8, 1) + pltpu.roll(ext, EXTRA - 16, 1))


def packed(lse):
    lane = lax.broadcasted_iota(jnp.int32, lse.shape, 1)
    hi, mid, low = (part.astype(jnp.float32) for part in split3(lse))
    out = jnp.where(lane < 8, hi, 0.0)
    out = jnp.where((lane >= 8) & (lane < 16), pltpu.roll(mid, 8, 1), out)
    out = jnp.where((lane >= 16) & (lane < 24), pltpu.roll(low, 16, 1), out)
    return out.astype(jnp.bfloat16)


def attention_body(meta, q_ref, kv_ref, sent_ref, kept_ref, *, block, group):
    step = pl.program_id(0)
    count = sent_ref.shape[1] - 1
    tokens = q_ref.shape[1]
    extent = kv_ref.shape[1]
    rank = meta[1]
    core = rank % 2
    seq = meta[0] + step
    first = rank * extent
    length = meta[2 + seq]
    c2 = LOG2E / math.sqrt(HD)
    lane = lax.broadcasted_iota(jnp.int32, (tokens, EXTRA), 1)

    def put(target, source, normal, lse):
        hi, mid, low = (part.astype(jnp.float32) for part in split3(lse))
        target[source, step] = normal
        old = target[source, count].astype(jnp.float32)
        old = jnp.where(step == 0, 0.0, old)
        old = jnp.where(lane == seq, hi, old)
        old = jnp.where(lane == seq + 8, mid, old)
        target[source, count] = jnp.where(lane == seq + 16, low, old).astype(jnp.bfloat16)

    def emit(normals, lses):
        for source in range(group // 2):
            pair = [(normals[2 * source + p], lses[2 * source + p]) for p in range(2)]
            picked = [jnp.where(core == 0, a, b) for a, b in zip(*pair)]
            other = [jnp.where(core == 0, b, a) for a, b in zip(*pair)]
            put(kept_ref, source, *picked)
            put(sent_ref, source, *other)

    def compute(masked):
        q = jnp.concatenate([q_ref[0, :, HD * h : HD * (h + 1)] for h in range(group)], axis=0)
        top = None
        for at in range(0, extent, block):
            scores = lax.dot_general(
                q,
                kv_ref[0, at : at + block, :HD],
                (((1,), (1,)), ((), ())),
                preferred_element_type=jnp.float32,
            )
            if masked:
                pos = first + at + lax.broadcasted_iota(jnp.int32, (tokens, block), 1)
                limit = length - tokens + lax.broadcasted_iota(jnp.int32, (tokens, block), 0)
                visible = jnp.concatenate([pos <= limit] * group, axis=0)
                scores = jnp.where(visible, scores, MASKED)
            here = jnp.max(scores, axis=1, keepdims=True)
            new_top = here if top is None else jnp.maximum(top, here)
            weights = jnp.exp2((scores - new_top) * c2)
            if masked:
                weights = jnp.where(visible, weights, 0.0)
            values = kv_ref[0, at : at + block, HD:]
            both = jnp.concatenate([values, jnp.ones_like(values)], axis=1)
            sums = jnp.dot(weights.astype(jnp.bfloat16), both, preferred_element_type=jnp.float32)
            part, part_total = sums[:, :HD], sums[:, HD:]
            if top is None:
                blended, totals = part, part_total
            else:
                shrink = jnp.exp2((top - new_top) * c2)
                blended = blended * shrink + part
                totals = totals * shrink + part_total
            top = new_top
        if masked:
            totals = jnp.where(totals > 0.0, totals, 1.0)
        normal = (blended / totals).astype(jnp.bfloat16)
        lse = top * c2 + jnp.log2(totals)
        cuts = [slice(tokens * h, tokens * (h + 1)) for h in range(group)]
        emit([normal[cut] for cut in cuts], [lse[cut] for cut in cuts])

    full = first + extent - 1 <= length - tokens
    hidden = first > length - 1

    @pl.when(full)
    def _():
        compute(False)

    @pl.when(jnp.logical_not(full | hidden))
    def _():
        compute(True)

    @pl.when(hidden)
    def _():
        zero = jnp.zeros((tokens, HD), jnp.bfloat16)
        nothing = jnp.full((tokens, EXTRA), MASKED, jnp.float32)
        emit([zero] * group, [nothing] * group)


def attention(meta, q, kv, group):
    count, tokens, width = q.shape
    extent = kv.shape[1]
    shape = (group // 2, count + 1, tokens, HD)
    whole = pl.BlockSpec(shape, lambda i, m: (0, 0, 0, 0))
    return pl.pallas_call(
        functools.partial(attention_body, block=256, group=group),
        grid_spec=pltpu.PrefetchScalarGridSpec(
            num_scalar_prefetch=1,
            grid=(count,),
            in_specs=[
                pl.BlockSpec((1, tokens, width), lambda i, m: (i, 0, 0)),
                pl.BlockSpec((1, extent, 2 * HD), lambda i, m: (m[0] + i, 0, 0)),
            ],
            out_specs=[whole, whole],
        ),
        out_shape=[jax.ShapeDtypeStruct(shape, jnp.bfloat16)] * 2,
        compiler_params=pltpu.CompilerParams(vmem_limit_bytes=40 * 1024 * 1024),
        cost_estimate=pl.CostEstimate(
            flops=count * tokens * group * extent * HD * 4,
            bytes_accessed=count * extent * 2 * HD * 2,
            transcendentals=count * tokens * group * extent,
        ),
        name="attend",
    )(meta, q, kv)


def merge_shares(parts):
    top = functools.reduce(jnp.maximum, parts)
    weights = [jnp.exp2(part - top) for part in parts]
    total = functools.reduce(jnp.add, weights)
    return [w / total for w in weights], top + jnp.log2(total)


VMEM = pl.BlockSpec(memory_space=pltpu.VMEM)
SMEM = pl.BlockSpec(memory_space=pltpu.SMEM)


def blend(blocks, shares, seq_lane):
    return functools.reduce(
        jnp.add,
        [b.astype(jnp.float32) * s[:, seq_lane : seq_lane + 1] for b, s in zip(blocks, shares)],
    )


def merge_pair_body(meta, *refs, halves, hops):
    outs = refs[-hops:]
    pairs = list(zip(refs[0:-hops:2], refs[1:-hops:2]))
    z, core = meta[0], meta[1]
    tokens = outs[0].shape[1]
    seqs = outs[0].shape[0] - 1
    half_len = seqs // 2
    lane = lax.broadcasted_iota(jnp.int32, (tokens, EXTRA), 1)
    for r in range(hops):
        chip = z ^ r
        joint = jnp.zeros((tokens, EXTRA), jnp.float32)
        for (a_ref, b_ref), (own_half, offset) in zip(pairs, halves):
            count = a_ref.shape[1] - 1
            ext = [joined(ref[chip, count].astype(jnp.float32)) for ref in (a_ref, b_ref)]
            shares, lse = merge_shares(ext)
            half = core if own_half else 1 - core
            start = half * half_len + offset
            joint = jnp.where((lane >= start) & (lane < start + count), lse, joint)
            for i in range(count):
                lanes = [c * half_len + offset + i for c in range(2)]
                picked = [
                    jnp.where(half == 0, s[:, lanes[0] : lanes[0] + 1], s[:, lanes[1] : lanes[1] + 1])
                    for s in shares
                ]
                outs[r][start + i] = (
                    a_ref[chip, i].astype(jnp.float32) * picked[0]
                    + b_ref[chip, i].astype(jnp.float32) * picked[1]
                ).astype(jnp.bfloat16)
        outs[r][seqs] = packed(joint)


def merge_pair(meta, pairs, halves, hops, seqs):
    tokens = pairs[0][0].shape[2]
    flat = [ref for pair in pairs for ref in pair]
    shape = jax.ShapeDtypeStruct((seqs + 1, tokens, HD), jnp.bfloat16)
    return pl.pallas_call(
        functools.partial(merge_pair_body, halves=halves, hops=hops),
        in_specs=[SMEM] + [VMEM] * len(flat),
        out_specs=[VMEM] * hops,
        out_shape=[shape] * hops,
        cost_estimate=pl.CostEstimate(flops=40_000_000, bytes_accessed=2_000_000, transcendentals=0),
        name="merge_pair",
    )(meta, *flat)


def merge_all_body(*refs):
    *parts, out_ref = refs
    seqs = out_ref.shape[0]
    shares, _ = merge_shares([joined(ref[seqs].astype(jnp.float32)) for ref in parts])
    for b in range(seqs):
        out_ref[b] = blend([ref[b] for ref in parts], shares, b).astype(jnp.bfloat16)


def merge_all(parts):
    seqs, tokens, width = parts[0].shape
    return pl.pallas_call(
        merge_all_body,
        in_specs=[VMEM] * len(parts),
        out_specs=VMEM,
        out_shape=jax.ShapeDtypeStruct((seqs - 1, tokens, width), jnp.bfloat16),
        cost_estimate=pl.CostEstimate(flops=20_000_000, bytes_accessed=600_000, transcendentals=0),
        name="merge_all",
    )(*parts)


def project_body(meta, *refs, count, adds):
    pieces, blocks = refs[:count], refs[count : 2 * count]
    rest = refs[2 * count :]
    w_ref = rest[-1]
    outs = rest[adds:-1]
    tokens = pieces[0].shape[2]
    half = pieces[0].shape[0]
    parity, rank, z = meta[0], meta[1], meta[2]
    for k in range(count):
        w_ref[k] = blocks[k][...]
    x = jnp.concatenate([ref[:, parity].reshape(half * tokens, HD) for ref in pieces], axis=1)
    w = jnp.concatenate([w_ref[rank ^ meta[3 + k]] for k in range(count)], axis=0)
    y = jnp.dot(x, w, preferred_element_type=jnp.float32)
    y = y.reshape(half, tokens, y.shape[1])
    if not adds:
        outs[0][...] = y.astype(jnp.bfloat16)
        return
    came = rest[0]
    for chip in range(half):
        total = y[chip] + came[chip].astype(jnp.float32)
        for r in range(half):
            @pl.when((z ^ r) == chip)
            def _(r=r, total=total):
                outs[r][...] = total.astype(jnp.bfloat16)


def project(meta, pieces, blocks, came=None):
    count = len(pieces)
    half, _, tokens, _ = pieces[0].shape
    width = blocks[0].shape[1]
    if came is None:
        out_shape = [jax.ShapeDtypeStruct((half, tokens, width), jnp.bfloat16)]
    else:
        out_shape = [jax.ShapeDtypeStruct((tokens, width), jnp.bfloat16)] * half
    more = [] if came is None else [came]
    return pl.pallas_call(
        functools.partial(project_body, count=count, adds=len(more)),
        in_specs=[SMEM] + [VMEM] * (2 * count + len(more)),
        out_specs=[VMEM] * len(out_shape),
        out_shape=out_shape,
        scratch_shapes=[pltpu.VMEM((count, HD, width), jnp.bfloat16)],
        cost_estimate=pl.CostEstimate(
            flops=2 * half * tokens * count * HD * width, bytes_accessed=3_000_000, transcendentals=0
        ),
        name="project",
    )(meta, *pieces, *blocks, *more)


def local(query, cache, head_of_slot, lengths, out_weight):
    seqs, tokens, width = query.shape
    group = width // HD
    half = seqs // 2
    seq_rank = lax.axis_index("seq")
    rank = lax.axis_index("tp")
    core, z = rank % 2, rank // 2
    tp_size = lax.axis_size("tp")
    chips = tp_size // 2
    seq_size = lax.axis_size("seq")
    head = head_of_slot[seq_rank]
    kv = cache.reshape(seqs, cache.shape[1], cache.shape[3])

    swap_core = [(i, i ^ 1) for i in range(tp_size)]
    flip, mirror = (lambda v: v ^ 1), (lambda v: chips - 1 - v)
    first_hop = [(2 * v + c, 2 * (flip, mirror)[c](v) + c) for v in range(chips) for c in range(2)]
    second_hop = [(2 * v + c, 2 * (mirror, flip)[c](v) + c) for v in range(chips) for c in range(2)]

    def cut(x, start, count):
        return lax.dynamic_slice_in_dim(x, start, count, 0)

    root = head // 2
    partner = jnp.where(core == 0, z ^ 1, chips - 1 - z)
    other = lax.ppermute(cut(query, core * half, half), "tp", swap_core)
    here = jnp.where(head % 2 == core, cut(query, (1 - core) * half, half), other)
    chunk = half // CHUNKS
    arrived = []
    for at in range(0, half, chunk):
        part = here[at : at + chunk]
        came = lax.ppermute(part, "tp", first_hop)
        part = jnp.where(partner == root, came, part)
        came = lax.ppermute(part, "tp", second_hop)
        arrived.append(jnp.where((z == root) | (partner == root), part, came))
    rest = [lax.ppermute(part, "tp", swap_core) for part in arrived]

    w = out_weight.reshape(group, HD, out_weight.shape[1])
    w, arrived = lax.optimization_barrier((w, arrived))
    pick = lambda j: lax.dynamic_index_in_dim(w, j, 0, keepdims=False)
    blocks = [pick(rank)] + [
        lax.ppermute(pick(rank ^ k), "tp", [(i, i ^ k) for i in range(tp_size)])
        for k in range(1, tp_size)
    ]

    facts = lambda start: jnp.concatenate([jnp.stack([start, rank]).astype(jnp.int32), lengths])
    first = [attention(facts((1 - core) * half + n * chunk), part, kv, group) for n, part in enumerate(arrived)]
    first_came = [lax.ppermute(sent, "tp", swap_core) for sent, _ in first]
    second = [
        attention(facts(core * half + n * chunk), rest[n], kv, group)
        for n in range(CHUNKS)
    ]
    second_came = [lax.ppermute(sent, "tp", swap_core) for sent, _ in second]
    pairs = [(second[n][1], first_came[n]) for n in range(CHUNKS)]
    pairs += [(first[n][1], second_came[n]) for n in range(CHUNKS)]
    halves = [(own, n * chunk) for own in (True, False) for n in range(CHUNKS)]
    spot = jnp.stack([z, core]).astype(jnp.int32)
    by_chip = merge_pair(spot, pairs, halves, chips, seqs)
    hops = [[(2 * v + c, 2 * (v ^ r) + c) for v in range(chips) for c in range(2)] for r in range(chips)]
    by_chip = [by_chip[0]] + [lax.ppermute(by_chip[r], "tp", hops[r]) for r in range(1, chips)]
    piece = merge_all(by_chip)

    pieces = [piece] + [
        lax.ppermute(piece, "seq", [(i, i ^ k) for i in range(seq_size)]) for k in range(1, seq_size)
    ]
    pieces = [p.reshape(chips, 2, tokens, HD) for p in pieces]
    heads = jnp.stack([head_of_slot[seq_rank ^ k] for k in range(seq_size)])
    note = lambda which: jnp.concatenate([jnp.stack([which, rank, z]), heads]).astype(jnp.int32)
    (sent,) = project(note(1 - core), pieces, blocks)
    came = lax.ppermute(sent, "tp", swap_core)
    sums = project(note(core), pieces, blocks, came)
    sums = [sums[0]] + [lax.ppermute(sums[r], "tp", hops[r]) for r in range(1, chips)]
    total = functools.reduce(jnp.add, [s.astype(jnp.float32) for s in sums])
    return total.astype(jnp.bfloat16)[None]


def solution(mesh):
    in_specs = (
        P("grp", None, "tp"),
        P("grp", "tp", "seq", None),
        P("grp"),
        P("grp"),
        P("tp", "seq"),
    )
    out_specs = P(("grp", "tp"), None, "seq")
    return jax.shard_map(local, mesh=mesh, in_specs=in_specs, out_specs=out_specs, check_vma=False)
```

```python
import functools
import math

import jax
import jax.numpy as jnp
from jax import lax
from jax.experimental import pallas as pl
from jax.experimental.pallas import tpu as pltpu
from jax.sharding import PartitionSpec as P


HD = 128
MASKED = -1e30
LOG2E = math.log2(math.e)
EXTRA = 128
CHUNKS = 2


def split3(x):
    hi = x.astype(jnp.bfloat16)
    rest = x - hi.astype(jnp.float32)
    mid = rest.astype(jnp.bfloat16)
    low = (rest - mid.astype(jnp.float32)).astype(jnp.bfloat16)
    return hi, mid, low


def joined(ext):
    return ext + (pltpu.roll(ext, EXTRA - 8, 1) + pltpu.roll(ext, EXTRA - 16, 1))


def packed(lse):
    lane = lax.broadcasted_iota(jnp.int32, lse.shape, 1)
    hi, mid, low = (part.astype(jnp.float32) for part in split3(lse))
    out = jnp.where(lane < 8, hi, 0.0)
    out = jnp.where((lane >= 8) & (lane < 16), pltpu.roll(mid, 8, 1), out)
    out = jnp.where((lane >= 16) & (lane < 24), pltpu.roll(low, 16, 1), out)
    return out.astype(jnp.bfloat16)


def attention_body(lengths, *refs, block, group, place):
    *q_refs, kv_ref, sent_ref, kept_ref = refs
    step = pl.program_id(0)
    count = sent_ref.shape[1] - 1
    tokens = q_refs[0].shape[1]
    chunk = q_refs[0].shape[0]
    extent = kv_ref.shape[1]
    rank = lax.axis_index("tp")
    core = rank % 2
    seq = place(core, step)
    first = rank * extent
    length = lengths[seq]
    c2 = LOG2E / math.sqrt(HD)
    lane = lax.broadcasted_iota(jnp.int32, (tokens, EXTRA), 1)

    def put(target, source, normal, lse):
        hi, mid, low = (part.astype(jnp.float32) for part in split3(lse))
        target[source, step] = normal
        old = target[source, count].astype(jnp.float32)
        old = jnp.where(step == 0, 0.0, old)
        old = jnp.where(lane == seq, hi, old)
        old = jnp.where(lane == seq + 8, mid, old)
        target[source, count] = jnp.where(lane == seq + 16, low, old).astype(jnp.bfloat16)

    def emit(normals, lses):
        for source in range(group // 2):
            pair = [(normals[2 * source + p], lses[2 * source + p]) for p in range(2)]
            picked = [jnp.where(core == 0, a, b) for a, b in zip(*pair)]
            other = [jnp.where(core == 0, b, a) for a, b in zip(*pair)]
            put(kept_ref, source, *picked)
            put(sent_ref, source, *other)

    def compute(masked):
        whole = q_refs[0][step % chunk]
        for n in range(1, len(q_refs)):
            whole = jnp.where(step >= n * chunk, q_refs[n][step % chunk], whole)
        q = jnp.concatenate([whole[:, HD * h : HD * (h + 1)] for h in range(group)], axis=0)

        def scored(at):
            return lax.dot_general(
                q,
                kv_ref[0, at : at + block, :HD],
                (((1,), (1,)), ((), ())),
                preferred_element_type=jnp.float32,
            )

        top = None
        upcoming = scored(0)
        for at in range(0, extent, block):
            scores = upcoming
            if at + block < extent:
                upcoming = scored(at + block)
            if masked:
                pos = first + at + lax.broadcasted_iota(jnp.int32, (tokens, block), 1)
                limit = length - tokens + lax.broadcasted_iota(jnp.int32, (tokens, block), 0)
                visible = jnp.concatenate([pos <= limit] * group, axis=0)
                scores = jnp.where(visible, scores, MASKED)
            here = jnp.max(scores, axis=1, keepdims=True)
            new_top = here if top is None else jnp.maximum(top, here)
            weights = jnp.exp2((scores - new_top) * c2)
            if masked:
                weights = jnp.where(visible, weights, 0.0)
            values = kv_ref[0, at : at + block, HD:]
            both = jnp.concatenate([values, jnp.ones_like(values)], axis=1)
            sums = jnp.dot(weights.astype(jnp.bfloat16), both, preferred_element_type=jnp.float32)
            part, part_total = sums[:, :HD], sums[:, HD:]
            if top is None:
                blended, totals = part, part_total
            else:
                shrink = jnp.exp2((top - new_top) * c2)
                blended = blended * shrink + part
                totals = totals * shrink + part_total
            top = new_top
        if masked:
            totals = jnp.where(totals > 0.0, totals, 1.0)
        normal = (blended / totals).astype(jnp.bfloat16)
        lse = top * c2 + jnp.log2(totals)
        cuts = [slice(tokens * h, tokens * (h + 1)) for h in range(group)]
        emit([normal[cut] for cut in cuts], [lse[cut] for cut in cuts])

    full = first + extent - 1 <= length - tokens
    hidden = first > length - 1

    @pl.when(full)
    def _():
        compute(False)

    @pl.when(jnp.logical_not(full | hidden))
    def _():
        compute(True)

    @pl.when(hidden)
    def _():
        zero = jnp.zeros((tokens, HD), jnp.bfloat16)
        nothing = jnp.full((tokens, EXTRA), MASKED, jnp.float32)
        emit([zero] * group, [nothing] * group)


def attention(lengths, parts, kv, group, place):
    chunk, tokens, _ = parts[0].shape
    count = chunk * len(parts)
    extent = kv.shape[1]
    shape = (group // 2, count + 1, tokens, HD)
    whole = pl.BlockSpec(memory_space=pltpu.VMEM)
    block_of = lambda i, m: (place(lax.axis_index("tp") % 2, i), 0, 0)
    return pl.pallas_call(
        functools.partial(attention_body, block=512, group=group, place=place),
        grid_spec=pltpu.PrefetchScalarGridSpec(
            num_scalar_prefetch=1,
            grid=(count,),
            in_specs=[whole] * len(parts) + [pl.BlockSpec((1, extent, 2 * HD), block_of)],
            out_specs=[whole, whole],
        ),
        out_shape=[jax.ShapeDtypeStruct(shape, jnp.bfloat16)] * 2,
        compiler_params=pltpu.CompilerParams(vmem_limit_bytes=50 * 1024 * 1024),
        cost_estimate=pl.CostEstimate(
            flops=count * tokens * group * extent * HD * 4,
            bytes_accessed=count * extent * 2 * HD * 2,
            transcendentals=count * tokens * group * extent,
        ),
        name="attend",
    )(lengths, *parts, kv)


def pack_rows_body(own_ref, other_ref, *outs):
    z = lax.axis_index("tp") // 2
    for r, out_ref in enumerate(outs):
        out_ref[0] = own_ref[z ^ (r + 1)]
        out_ref[1] = other_ref[z ^ (r + 1)]


def pack_rows(own, other):
    shape = jax.ShapeDtypeStruct((2,) + own.shape[1:], own.dtype)
    return small_call(pack_rows_body, [own, other], [shape] * (own.shape[0] - 1), 5_000_000)


def split_rows_body(w_ref, own_ref, other_ref):
    core = lax.axis_index("tp") % 2
    for v in range(w_ref.shape[0]):
        own_ref[v] = w_ref[v, core]
        other_ref[v] = w_ref[v, 1 - core]


def split_rows(w):
    shape = jax.ShapeDtypeStruct((w.shape[0],) + w.shape[2:], w.dtype)
    return small_call(split_rows_body, [w], [shape, shape], 5_000_000)


def cut_query_body(q_ref, *refs, chunks):
    *outs, sems = refs
    core = lax.axis_index("tp") % 2
    count = outs[0].shape[0]
    half = count * chunks
    copies = []
    for n, half_of in enumerate((core, 1 - core)):
        for k in range(chunks):
            source = q_ref.at[pl.ds(half_of * half + k * count, count)]
            copies.append(pltpu.make_async_copy(source, outs[n * chunks + k], sems.at[n, k]))
    for copy in copies:
        copy.start()
    for copy in copies:
        copy.wait()


def cut_query(query, chunks):
    shape = jax.ShapeDtypeStruct((query.shape[0] // (2 * chunks),) + query.shape[1:], query.dtype)
    return pl.pallas_call(
        functools.partial(cut_query_body, chunks=chunks),
        in_specs=[pl.BlockSpec(memory_space=pltpu.HBM)],
        out_specs=[pl.BlockSpec(memory_space=pltpu.VMEM)] * (2 * chunks),
        out_shape=[shape] * (2 * chunks),
        scratch_shapes=[pltpu.SemaphoreType.DMA((2, chunks))],
        compiler_params=pltpu.CompilerParams(vmem_limit_bytes=24 * 1024 * 1024),
        cost_estimate=pl.CostEstimate(flops=1_000_000, bytes_accessed=4 * query.size, transcendentals=0),
        name="cut_query",
    )(query)


def choose_body(head_of_slot, a_ref, b_ref, out_ref, *, first):
    rank = lax.axis_index("tp")
    head = head_of_slot[lax.axis_index("seq")]
    take_first = first(rank % 2, rank // 2, head)

    @pl.when(take_first)
    def _():
        out_ref[...] = a_ref[...]

    @pl.when(jnp.logical_not(take_first))
    def _():
        out_ref[...] = b_ref[...]


def choose(head_of_slot, a, b, first):
    shape = jax.ShapeDtypeStruct(a.shape, a.dtype)
    body = functools.partial(choose_body, first=first)
    return small_call(body, [a, b], [shape], 1_000_000, prefetch=(head_of_slot,))[0]


def merge_shares(parts):
    top = functools.reduce(jnp.maximum, parts)
    weights = [jnp.exp2(part - top) for part in parts]
    total = functools.reduce(jnp.add, weights)
    return [w / total for w in weights], top + jnp.log2(total)


def small_call(body, operands, out_shape, flops, prefetch=(), scratch=()):
    whole = pl.BlockSpec(memory_space=pltpu.VMEM)

    return pl.pallas_call(
        body,
        grid_spec=pltpu.PrefetchScalarGridSpec(
            num_scalar_prefetch=len(prefetch),
            grid=(1,),
            in_specs=[whole] * len(operands),
            out_specs=[whole] * len(out_shape),
            scratch_shapes=list(scratch),
        ),
        out_shape=out_shape,
        compiler_params=pltpu.CompilerParams(vmem_limit_bytes=24 * 1024 * 1024),
        cost_estimate=pl.CostEstimate(flops=flops, bytes_accessed=2_000_000, transcendentals=0),
    )(*prefetch, *operands)


def merge_pair_body(*refs, groups, chips):
    *refs, out_ref = refs
    core = lax.axis_index("tp") % 2
    tokens = out_ref.shape[2]
    seqs = out_ref.shape[1] - 1
    half_len = seqs // 2
    lane = lax.broadcasted_iota(jnp.int32, (tokens, EXTRA), 1)
    for chip in range(chips):
        ext = [joined(ref[chip, ref.shape[1] - 1].astype(jnp.float32)) for ref in refs]
        joint = jnp.zeros((tokens, EXTRA), jnp.float32)
        for a, a_at, b, b_at, own_half, offset, count in groups:
            shares, lse = merge_shares([ext[a], ext[b]])
            half = core if own_half else 1 - core
            start = half * half_len + offset
            joint = jnp.where((lane >= start) & (lane < start + count), lse, joint)
            share = jnp.where(half == 0, shares[0], pltpu.roll(shares[0], EXTRA - half_len, 1))
            for i in range(count):
                kept = refs[a][chip, a_at + i].astype(jnp.float32)
                came = refs[b][chip, b_at + i].astype(jnp.float32)
                out_ref[chip, start + i] = (
                    came + (kept - came) * share[:, offset + i : offset + i + 1]
                ).astype(jnp.bfloat16)
        out_ref[chip, seqs] = packed(joint)


def merge_pair(parts, groups, seqs):
    chips, _, tokens, _ = parts[0].shape
    return small_call(
        functools.partial(merge_pair_body, groups=groups, chips=chips),
        parts,
        [jax.ShapeDtypeStruct((chips, seqs + 1, tokens, HD), jnp.bfloat16)],
        40_000_000,
    )[0]


def merge_all_body(x_ref, out_ref):
    count, seqs = x_ref.shape[0], out_ref.shape[0]
    shares, _ = merge_shares([joined(x_ref[k, seqs].astype(jnp.float32)) for k in range(count)])
    for b in range(seqs):
        parts = [x_ref[k, b].astype(jnp.float32) * shares[k][:, b : b + 1] for k in range(count)]
        out_ref[b] = functools.reduce(jnp.add, parts).astype(jnp.bfloat16)


def merge_all(x):
    _, seqs, tokens, width = x.shape
    return small_call(
        merge_all_body, [x], [jax.ShapeDtypeStruct((seqs - 1, tokens, width), jnp.bfloat16)], 20_000_000
    )[0]


def project_body(head_of_slot, *refs, count, own_parity):
    pieces = refs[:count]
    own_ref, came_ref, flip_ref, far_ref, far_hop_ref, mirror_ref, out_ref, w_ref = refs[count:]
    tokens = pieces[0].shape[2]
    half = pieces[0].shape[0]
    seq_rank = lax.axis_index("seq")
    rank = lax.axis_index("tp")
    core, z = rank % 2, rank // 2
    parity = core if own_parity else 1 - core
    w_ref[0, 0] = own_ref[z]
    w_ref[0, 1] = came_ref[z]
    w_ref[1] = flip_ref[...]
    w_ref[half - 1] = mirror_ref[...]

    @pl.when(core == 0)
    def _():
        w_ref[2] = far_ref[...]

    @pl.when(core == 1)
    def _():
        w_ref[2] = far_hop_ref[...]

    x = jnp.concatenate([ref[:, parity].reshape(half * tokens, HD) for ref in pieces], axis=1)
    rows = []
    for k in range(count):
        head = head_of_slot[seq_rank ^ k]
        rows.append(w_ref[(head // 2) ^ z, (head % 2) ^ core])
    y = jnp.dot(x, jnp.concatenate(rows, axis=0), preferred_element_type=jnp.float32)
    out_ref[...] = y.reshape(out_ref.shape).astype(out_ref.dtype)


def project(head_of_slot, pieces, blocks, own_parity, dtype):
    count = len(pieces)
    half, _, tokens, _ = pieces[0].shape
    width = blocks[0].shape[-1]
    return small_call(
        functools.partial(project_body, count=count, own_parity=own_parity),
        [*pieces, *blocks],
        [jax.ShapeDtypeStruct((half, tokens, width), dtype)],
        2 * half * tokens * count * HD * width,
        prefetch=(head_of_slot,),
        scratch=[pltpu.VMEM((half, 2, HD, width), jnp.bfloat16)],
    )[0]


def layer(query, cache, head_of_slot, lengths, out_weight):
    seqs, tokens, width = query.shape
    group = width // HD
    half = seqs // 2
    tp_size = lax.axis_size("tp")
    chips = tp_size // 2
    seq_size = lax.axis_size("seq")
    kv = cache.reshape(seqs, cache.shape[1], cache.shape[3])

    def send(x, axis, pairs):
        return lax.ppermute(x, axis, pairs)

    ring = range(chips)
    swap_core = [(i, i ^ 1) for i in range(tp_size)]
    to_flip = [(2 * v + c, 2 * (v ^ 1) + c) for v in ring for c in range(2)]
    to_mirror = [(2 * v + c, 2 * (chips - 1 - v) + c) for v in ring for c in range(2)]
    first_hop = to_flip[0::2] + to_mirror[1::2]
    second_hop = to_mirror[0::2] + to_flip[1::2]

    def partner(core, z):
        return jnp.where(core == 0, z ^ 1, chips - 1 - z)

    def owned(core, z, head):
        return head % 2 == core

    def unreached(core, z, head):
        return partner(core, z) != head // 2

    def reached(core, z, head):
        return (z == head // 2) | (partner(core, z) == head // 2)

    chunk = half // CHUNKS
    cuts = cut_query(query, CHUNKS)
    came = [send(cuts[n], "tp", swap_core) for n in range(CHUNKS)]
    parts = [choose(head_of_slot, cuts[CHUNKS + n], new, owned) for n, new in enumerate(came)]
    came = [send(part, "tp", first_hop) for part in parts]
    parts = [choose(head_of_slot, part, new, unreached) for new, part in zip(came, parts)]
    came = [send(part, "tp", second_hop) for part in parts]
    parts = [choose(head_of_slot, part, new, reached) for new, part in zip(came, parts)]
    rest = [send(part, "tp", swap_core) for part in parts]
    own, other = split_rows(out_weight.reshape(chips, 2, HD, out_weight.shape[1]))
    swapped = send(other, "tp", swap_core)
    for_flip, for_far, for_mirror = pack_rows(own, swapped)
    flipped = send(for_flip, "tp", to_flip)
    mirrored = send(for_mirror, "tp", to_mirror)
    down = [(2 * v + 1, 2 * ((v - 1) % chips) + 1) for v in ring]
    far = send(for_far, "tp", [(2 * v, 2 * (v ^ 2)) for v in ring] + down)
    far_hop = send(far, "tp", down)
    blocks = [own, swapped, flipped, far, far_hop, mirrored]

    left = half - chunk

    def later(core, step):
        own_half = (1 - core) * half + chunk + step
        return jnp.where(step < left, own_half, core * half + step - left)

    first = attention(lengths, parts[:1], kv, group, lambda core, step: (1 - core) * half + step)
    first_came = send(first[0], "tp", swap_core)
    second = attention(lengths, parts[1:] + rest, kv, group, later)
    second_came = send(second[0], "tp", swap_core)
    groups = (
        (2, left, 1, 0, True, 0, chunk),
        (2, half, 3, 0, True, chunk, left),
        (0, 0, 3, left, False, 0, chunk),
        (2, 0, 3, half, False, chunk, left),
    )
    by_chip = merge_pair([first[1], first_came, second[1], second_came], groups, seqs)
    z_groups = [[2 * v + c for v in ring] for c in range(2)]

    def spread(x):
        return lax.all_to_all(x, "tp", 0, 0, tiled=True, axis_index_groups=z_groups)

    piece = merge_all(spread(by_chip))

    pieces = [piece] + [send(piece, "seq", [(i, i ^ k) for i in range(seq_size)]) for k in range(1, seq_size)]
    pieces = [p.reshape(chips, 2, tokens, HD) for p in pieces]
    sent = project(head_of_slot, pieces, blocks, False, jnp.bfloat16)
    came = send(sent, "tp", swap_core)
    kept = project(head_of_slot, pieces, blocks, True, jnp.float32)
    sums = (kept + came.astype(jnp.float32)).astype(jnp.bfloat16)
    arrived = spread(sums)
    return jnp.sum(arrived.astype(jnp.float32), axis=0, keepdims=True).astype(jnp.bfloat16)


def solution(mesh):
    in_specs = (
        P("grp", None, "tp"),
        P("grp", "tp", "seq", None),
        P("grp"),
        P("grp"),
        P("tp", "seq"),
    )
    out_specs = P(("grp", "tp"), None, "seq")
    return jax.shard_map(layer, mesh=mesh, in_specs=in_specs, out_specs=out_specs, check_vma=False)
```

```python
import functools
import math

import jax
import jax.numpy as jnp
from jax import lax
from jax.experimental import pallas as pl
from jax.experimental.pallas import tpu as pltpu
from jax.sharding import PartitionSpec as P


HD = 128
MASKED = -1e30
LOG2E = math.log2(math.e)
EXTRA = 128
CHUNKS = 2


def split3(x):
    hi = x.astype(jnp.bfloat16)
    rest = x - hi.astype(jnp.float32)
    mid = rest.astype(jnp.bfloat16)
    low = (rest - mid.astype(jnp.float32)).astype(jnp.bfloat16)
    return hi, mid, low


def joined(ext):
    return ext + (pltpu.roll(ext, EXTRA - 8, 1) + pltpu.roll(ext, EXTRA - 16, 1))


def packed(lse):
    lane = lax.broadcasted_iota(jnp.int32, lse.shape, 1)
    hi, mid, low = (part.astype(jnp.float32) for part in split3(lse))
    out = jnp.where(lane < 8, hi, 0.0)
    out = jnp.where((lane >= 8) & (lane < 16), pltpu.roll(mid, 8, 1), out)
    out = jnp.where((lane >= 16) & (lane < 24), pltpu.roll(low, 16, 1), out)
    return out.astype(jnp.bfloat16)


def attention_body(lengths, *refs, block, group, place):
    *q_refs, kv_ref, sent_ref, kept_ref = refs
    step = pl.program_id(0)
    count = sent_ref.shape[1] - 1
    tokens = q_refs[0].shape[1]
    chunk = q_refs[0].shape[0]
    extent = kv_ref.shape[1]
    rank = lax.axis_index("tp")
    core = rank % 2
    seq = place(core, step)
    first = rank * extent
    length = lengths[seq]
    c2 = LOG2E / math.sqrt(HD)
    lane = lax.broadcasted_iota(jnp.int32, (tokens, EXTRA), 1)

    def put(target, source, normal, lse):
        hi, mid, low = (part.astype(jnp.float32) for part in split3(lse))
        target[source, step] = normal
        old = target[source, count].astype(jnp.float32)
        old = jnp.where(step == 0, 0.0, old)
        old = jnp.where(lane == seq, hi, old)
        old = jnp.where(lane == seq + 8, mid, old)
        target[source, count] = jnp.where(lane == seq + 16, low, old).astype(jnp.bfloat16)

    def emit(normals, lses):
        for source in range(group // 2):
            pair = [(normals[2 * source + p], lses[2 * source + p]) for p in range(2)]
            picked = [jnp.where(core == 0, a, b) for a, b in zip(*pair)]
            other = [jnp.where(core == 0, b, a) for a, b in zip(*pair)]
            put(kept_ref, source, *picked)
            put(sent_ref, source, *other)

    def compute(masked):
        whole = q_refs[0][step % chunk]
        for n in range(1, len(q_refs)):
            whole = jnp.where(step >= n * chunk, q_refs[n][step % chunk], whole)
        q = jnp.concatenate([whole[:, HD * h : HD * (h + 1)] for h in range(group)], axis=0)

        def scored(at):
            return lax.dot_general(
                q,
                kv_ref[seq, at : at + block, :HD],
                (((1,), (1,)), ((), ())),
                preferred_element_type=jnp.float32,
            )

        top = None
        upcoming = scored(0)
        for at in range(0, extent, block):
            scores = upcoming
            if at + block < extent:
                upcoming = scored(at + block)
            if masked:
                pos = first + at + lax.broadcasted_iota(jnp.int32, (tokens, block), 1)
                limit = length - tokens + lax.broadcasted_iota(jnp.int32, (tokens, block), 0)
                visible = jnp.concatenate([pos <= limit] * group, axis=0)
                scores = jnp.where(visible, scores, MASKED)
            here = jnp.max(scores, axis=1, keepdims=True)
            new_top = here if top is None else jnp.maximum(top, here)
            weights = jnp.exp2((scores - new_top) * c2)
            if masked:
                weights = jnp.where(visible, weights, 0.0)
            values = kv_ref[seq, at : at + block, HD:]
            both = jnp.concatenate([values, jnp.ones_like(values)], axis=1)
            sums = jnp.dot(weights.astype(jnp.bfloat16), both, preferred_element_type=jnp.float32)
            part, part_total = sums[:, :HD], sums[:, HD:]
            if top is None:
                blended, totals = part, part_total
            else:
                shrink = jnp.exp2((top - new_top) * c2)
                blended = blended * shrink + part
                totals = totals * shrink + part_total
            top = new_top
        if masked:
            totals = jnp.where(totals > 0.0, totals, 1.0)
        normal = (blended / totals).astype(jnp.bfloat16)
        lse = top * c2 + jnp.log2(totals)
        cuts = [slice(tokens * h, tokens * (h + 1)) for h in range(group)]
        emit([normal[cut] for cut in cuts], [lse[cut] for cut in cuts])

    full = first + extent - 1 <= length - tokens
    hidden = first > length - 1

    @pl.when(full)
    def _():
        compute(False)

    @pl.when(jnp.logical_not(full | hidden))
    def _():
        compute(True)

    @pl.when(hidden)
    def _():
        zero = jnp.zeros((tokens, HD), jnp.bfloat16)
        nothing = jnp.full((tokens, EXTRA), MASKED, jnp.float32)
        emit([zero] * group, [nothing] * group)


def attention(lengths, parts, kv, group, place):
    chunk, tokens, _ = parts[0].shape
    count = chunk * len(parts)
    extent = kv.shape[1]
    shape = (group // 2, count + 1, tokens, HD)
    whole = pl.BlockSpec(memory_space=pltpu.VMEM)
    return pl.pallas_call(
        functools.partial(attention_body, block=512, group=group, place=place),
        grid_spec=pltpu.PrefetchScalarGridSpec(
            num_scalar_prefetch=1,
            grid=(count,),
            in_specs=[whole] * (len(parts) + 1),
            out_specs=[whole, whole],
        ),
        out_shape=[jax.ShapeDtypeStruct(shape, jnp.bfloat16)] * 2,
        compiler_params=pltpu.CompilerParams(vmem_limit_bytes=36 * 1024 * 1024),
        cost_estimate=pl.CostEstimate(
            flops=count * tokens * group * extent * HD * 4,
            bytes_accessed=count * extent * 2 * HD * 2,
            transcendentals=count * tokens * group * extent,
        ),
        name="attend",
    )(lengths, *parts, kv)


def pack_rows_body(own_ref, other_ref, *outs):
    z = lax.axis_index("tp") // 2
    for r, out_ref in enumerate(outs):
        out_ref[0] = own_ref[z ^ (r + 1)]
        out_ref[1] = other_ref[z ^ (r + 1)]


def pack_rows(own, other):
    shape = jax.ShapeDtypeStruct((2,) + own.shape[1:], own.dtype)
    return small_call(pack_rows_body, [own, other], [shape] * (own.shape[0] - 1), 5_000_000)


def cut_query_body(q_ref, *cuts, chunks):
    core = lax.axis_index("tp") % 2
    count = cuts[0].shape[0]
    for n, half in enumerate((core, 1 - core)):
        for k in range(chunks):
            cuts[n * chunks + k][...] = q_ref[pl.ds((half * chunks + k) * count, count)]


def cut_query(query, chunks):
    cut = jax.ShapeDtypeStruct((query.shape[0] // (2 * chunks),) + query.shape[1:], query.dtype)
    body = functools.partial(cut_query_body, chunks=chunks)
    return small_call(body, [query], [cut] * (2 * chunks), 1_000_000)


def flag_body(head_of_slot, flag_ref, *, tests):
    rank = lax.axis_index("tp")
    head = head_of_slot[lax.axis_index("seq")]
    for n, test in enumerate(tests):
        outcome = jnp.where(test(rank % 2, rank // 2, head), 1, 0)
        flag_ref[n] = jnp.full(flag_ref.shape[1:], outcome, jnp.int32)


def flag(head_of_slot, tests):
    flags = jax.ShapeDtypeStruct((len(tests), 8, 128), jnp.int32)
    body = functools.partial(flag_body, tests=tests)
    return small_call(body, [], [flags], 1_000, prefetch=(head_of_slot,))[0]


def split_rows_body(w_ref, own_ref, other_ref):
    core = lax.axis_index("tp") % 2
    for v in range(w_ref.shape[0]):
        own_ref[v] = w_ref[v, core]
        other_ref[v] = w_ref[v, 1 - core]


def split_rows(w):
    rows = jax.ShapeDtypeStruct((w.shape[0],) + w.shape[2:], w.dtype)
    return small_call(split_rows_body, [w], [rows, rows], 5_000_000)


def choose_body(flag_ref, a_ref, b_ref, out_ref, *, which):
    take_first = jnp.max(flag_ref[which]) > 0

    @pl.when(take_first)
    def _():
        out_ref[...] = a_ref[...]

    @pl.when(jnp.logical_not(take_first))
    def _():
        out_ref[...] = b_ref[...]


def choose(flags, a, b, which):
    shape = jax.ShapeDtypeStruct(a.shape, a.dtype)
    body = functools.partial(choose_body, which=which)
    return small_call(body, [flags, a, b], [shape], 1_000_000)[0]


def merge_shares(parts):
    top = functools.reduce(jnp.maximum, parts)
    weights = [jnp.exp2(part - top) for part in parts]
    total = functools.reduce(jnp.add, weights)
    return [w / total for w in weights], top + jnp.log2(total)


def small_call(body, operands, out_shape, flops, prefetch=(), scratch=()):
    whole = pl.BlockSpec(memory_space=pltpu.VMEM)

    return pl.pallas_call(
        body,
        grid_spec=pltpu.PrefetchScalarGridSpec(
            num_scalar_prefetch=len(prefetch),
            grid=(1,),
            in_specs=[whole] * len(operands),
            out_specs=[whole] * len(out_shape),
            scratch_shapes=list(scratch),
        ),
        out_shape=out_shape,
        compiler_params=pltpu.CompilerParams(vmem_limit_bytes=24 * 1024 * 1024),
        cost_estimate=pl.CostEstimate(flops=flops, bytes_accessed=2_000_000, transcendentals=0),
    )(*prefetch, *operands)


def merge_pair_body(*refs, groups, chips):
    *refs, out_ref = refs
    core = lax.axis_index("tp") % 2
    tokens = out_ref.shape[2]
    seqs = out_ref.shape[1] - 1
    half_len = seqs // 2
    lane = lax.broadcasted_iota(jnp.int32, (tokens, EXTRA), 1)
    for chip in range(chips):
        ext = [joined(ref[chip, ref.shape[1] - 1].astype(jnp.float32)) for ref in refs]
        joint = jnp.zeros((tokens, EXTRA), jnp.float32)
        for a, a_at, b, b_at, own_half, offset, count in groups:
            shares, lse = merge_shares([ext[a], ext[b]])
            half = core if own_half else 1 - core
            start = half * half_len + offset
            joint = jnp.where((lane >= start) & (lane < start + count), lse, joint)
            share = jnp.where(half == 0, shares[0], pltpu.roll(shares[0], EXTRA - half_len, 1))
            for i in range(count):
                kept = refs[a][chip, a_at + i].astype(jnp.float32)
                came = refs[b][chip, b_at + i].astype(jnp.float32)
                out_ref[chip, start + i] = (
                    came + (kept - came) * share[:, offset + i : offset + i + 1]
                ).astype(jnp.bfloat16)
        out_ref[chip, seqs] = packed(joint)


def merge_pair(parts, groups, seqs):
    chips, _, tokens, _ = parts[0].shape
    return small_call(
        functools.partial(merge_pair_body, groups=groups, chips=chips),
        parts,
        [jax.ShapeDtypeStruct((chips, seqs + 1, tokens, HD), jnp.bfloat16)],
        40_000_000,
    )[0]


def merge_all_body(x_ref, out_ref):
    count, seqs = x_ref.shape[0], out_ref.shape[0]
    shares, _ = merge_shares([joined(x_ref[k, seqs].astype(jnp.float32)) for k in range(count)])
    for b in range(seqs):
        parts = [x_ref[k, b].astype(jnp.float32) * shares[k][:, b : b + 1] for k in range(count)]
        out_ref[b] = functools.reduce(jnp.add, parts).astype(jnp.bfloat16)


def merge_all(x):
    _, seqs, tokens, width = x.shape
    return small_call(
        merge_all_body, [x], [jax.ShapeDtypeStruct((seqs - 1, tokens, width), jnp.bfloat16)], 20_000_000
    )[0]


def assemble_body(head_of_slot, own_ref, came_ref, flip_ref, far_ref, far_hop_ref, mirror_ref, out_ref, w_ref):
    half = own_ref.shape[0]
    seq_rank = lax.axis_index("seq")
    rank = lax.axis_index("tp")
    core, z = rank % 2, rank // 2
    w_ref[0, 0] = own_ref[z]
    w_ref[0, 1] = came_ref[z]
    w_ref[1] = flip_ref[...]
    w_ref[half - 1] = mirror_ref[...]

    @pl.when(core == 0)
    def _():
        w_ref[2] = far_ref[...]

    @pl.when(core == 1)
    def _():
        w_ref[2] = far_hop_ref[...]

    for k in range(2 * half):
        head = head_of_slot[seq_rank ^ k]
        out_ref[HD * k : HD * (k + 1)] = w_ref[(head // 2) ^ z, (head % 2) ^ core]


def assemble(head_of_slot, blocks):
    half, _, width = blocks[0].shape
    return small_call(
        assemble_body,
        blocks,
        [jax.ShapeDtypeStruct((2 * half * HD, width), jnp.bfloat16)],
        5_000_000,
        prefetch=(head_of_slot,),
        scratch=[pltpu.VMEM((half, 2, HD, width), jnp.bfloat16)],
    )[0]


def project_body(*refs, own_parity):
    *pieces, w_ref, out_ref = refs
    half, _, tokens, _ = pieces[0].shape
    core = lax.axis_index("tp") % 2
    parity = core if own_parity else 1 - core
    x = jnp.concatenate([ref[:, parity].reshape(half * tokens, HD) for ref in pieces], axis=1)
    y = jnp.dot(x, w_ref[...], preferred_element_type=jnp.float32)
    out_ref[...] = y.reshape(out_ref.shape).astype(out_ref.dtype)


def project(pieces, w, own_parity, dtype):
    half, _, tokens, _ = pieces[0].shape
    return small_call(
        functools.partial(project_body, own_parity=own_parity),
        [*pieces, w],
        [jax.ShapeDtypeStruct((half, tokens, w.shape[1]), dtype)],
        2 * half * tokens * w.size,
    )[0]


def layer(query, cache, head_of_slot, lengths, out_weight):
    seqs, tokens, width = query.shape
    group = width // HD
    half = seqs // 2
    tp_size = lax.axis_size("tp")
    chips = tp_size // 2
    seq_size = lax.axis_size("seq")
    kv = cache.reshape(seqs, cache.shape[1], cache.shape[3])

    def send(x, axis, pairs):
        return lax.ppermute(x, axis, pairs)

    ring = range(chips)
    swap_core = [(i, i ^ 1) for i in range(tp_size)]
    to_flip = [(2 * v + c, 2 * (v ^ 1) + c) for v in ring for c in range(2)]
    to_mirror = [(2 * v + c, 2 * (chips - 1 - v) + c) for v in ring for c in range(2)]
    first_hop = to_flip[0::2] + to_mirror[1::2]
    second_hop = to_mirror[0::2] + to_flip[1::2]

    def partner(core, z):
        return jnp.where(core == 0, z ^ 1, chips - 1 - z)

    def owned(core, z, head):
        return head % 2 == core

    def unreached(core, z, head):
        return partner(core, z) != head // 2

    def reached(core, z, head):
        return (z == head // 2) | (partner(core, z) == head // 2)

    chunk = half // CHUNKS
    cuts = cut_query(query, CHUNKS)
    flags = flag(head_of_slot, (owned, unreached, reached))
    came = [send(cuts[n], "tp", swap_core) for n in range(CHUNKS)]
    parts = [choose(flags, cuts[CHUNKS + n], new, 0) for n, new in enumerate(came)]
    came = [send(part, "tp", first_hop) for part in parts]
    parts = [choose(flags, part, new, 1) for new, part in zip(came, parts)]
    came = [send(part, "tp", second_hop) for part in parts]
    parts = [choose(flags, part, new, 2) for new, part in zip(came, parts)]
    rest = [send(part, "tp", swap_core) for part in parts]
    own, other = split_rows(out_weight.reshape(chips, 2, HD, out_weight.shape[1]))
    swapped = send(other, "tp", swap_core)
    for_flip, for_far, for_mirror = pack_rows(own, swapped)
    flipped = send(for_flip, "tp", to_flip)
    mirrored = send(for_mirror, "tp", to_mirror)
    down = [(2 * v + 1, 2 * ((v - 1) % chips) + 1) for v in ring]
    far = send(for_far, "tp", [(2 * v, 2 * (v ^ 2)) for v in ring] + down)
    far_hop = send(far, "tp", down)
    blocks = [own, swapped, flipped, far, far_hop, mirrored]

    left = half - chunk

    def later(core, step):
        own_half = (1 - core) * half + chunk + step
        return jnp.where(step < left, own_half, core * half + chunk + step - left)

    first = attention(lengths, parts[:1], kv, group, lambda core, step: (1 - core) * half + step)
    first_came = send(first[0], "tp", swap_core)
    second = attention(lengths, rest[:1], kv, group, lambda core, step: core * half + step)
    second_came = send(second[0], "tp", swap_core)
    third = attention(lengths, parts[1:] + rest[1:], kv, group, later)
    third_came = send(third[0], "tp", swap_core)
    groups = (
        (2, 0, 1, 0, True, 0, chunk),
        (4, left, 5, 0, True, chunk, left),
        (0, 0, 3, 0, False, 0, chunk),
        (4, 0, 5, left, False, chunk, left),
    )
    by_chip = merge_pair(
        [first[1], first_came, second[1], second_came, third[1], third_came], groups, seqs
    )
    z_groups = [[2 * v + c for v in ring] for c in range(2)]

    def spread(x):
        return lax.all_to_all(x, "tp", 0, 0, tiled=True, axis_index_groups=z_groups)

    piece = merge_all(spread(by_chip))

    pieces = [piece] + [send(piece, "seq", [(i, i ^ k) for i in range(seq_size)]) for k in range(1, seq_size)]
    pieces = [p.reshape(chips, 2, tokens, HD) for p in pieces]
    w = assemble(head_of_slot, blocks)
    sent = project(pieces, w, False, jnp.bfloat16)
    came = send(sent, "tp", swap_core)
    kept = project(pieces, w, True, jnp.float32)
    sums = (kept + came.astype(jnp.float32)).astype(jnp.bfloat16)
    arrived = spread(sums)
    return jnp.sum(arrived.astype(jnp.float32), axis=0, keepdims=True).astype(jnp.bfloat16)


def solution(mesh):
    in_specs = (
        P("grp", None, "tp"),
        P("grp", "tp", "seq", None),
        P("grp"),
        P("grp"),
        P("tp", "seq"),
    )
    out_specs = P(("grp", "tp"), None, "seq")
    return jax.shard_map(layer, mesh=mesh, in_specs=in_specs, out_specs=out_specs, check_vma=False)
```
